128 devices in a mesh: rep: 1, data: 16 (over z, y), expert: 8 (over x, core).
Axes of the slice: x: 4, y: 4, z: 4, core: 2. Of those that a mesh axis runs over, the one named last changes fastest.
Arguments:
- x: bfloat16 [65536, 2048], P(('rep', 'expert', 'data'))
- expert_idx: int32 [65536, 2], P(('rep', 'expert', 'data'))
- gate: float32 [65536, 2], P(('rep', 'expert', 'data'))
- w_gate: bfloat16 [8, 2048, 5632], P('expert', 'data')
- w_up: bfloat16 [8, 2048, 5632], P('expert', 'data')
- w_down: bfloat16 [8, 5632, 2048], P('expert', None, 'data')
Outputs:
- output: bfloat16 [65536, 2048], P(('rep', 'expert', 'data'))
All inputs are finite; a program needn't handle non-finite values.
Results may differ from the reference program's by a relative error of at most 0.001.
Values are sent between devices in bfloat16 or wider.
A program may use at most 1 GiB of HBM per device.

```python
import jax
import jax.numpy as jnp
from jax import lax

TOK_DEV = 512
D_MODEL = 2048
FFN = 5632
EXPERTS = 8
TOP_K = 2
EP_SIZE = 8
DP_SIZE = 16
CAPACITY = 160


def route_ids(key):
    n_blocks = EP_SIZE * DP_SIZE
    key_bias, key_hot, key_score = jax.random.split(key, 3)
    expert_bias = jax.random.randint(key_bias, (EXPERTS,), 0, 2 ** 20, dtype=jnp.int32)
    hot_expert = jax.random.randint(key_hot, (), 0, EXPERTS, dtype=jnp.int32)
    scores = jax.random.randint(key_score, (n_blocks, TOK_DEV, EXPERTS), 0, 2 ** 20, dtype=jnp.int32) + expert_bias
    forced = (jnp.arange(TOK_DEV) < CAPACITY)[None, :, None] & (jnp.arange(EXPERTS) == hot_expert)[None, None, :]
    scores = (scores + forced.astype(jnp.int32) * 2 ** 21) * EXPERTS + jnp.arange(EXPERTS, dtype=jnp.int32)
    chosen = lax.top_k(scores, TOP_K)[1]
    return chosen.reshape(n_blocks * TOK_DEV, TOP_K).astype(jnp.int32)


def setup_inputs(seed: int = 0, part: int = 0) -> dict:
    key_shared, key_local = jax.random.split(jax.random.key(seed))
    key_tok, key_route, key_gate = jax.random.split(jax.random.fold_in(key_local, part), 3)
    key_wg, key_wu, key_wd = jax.random.split(key_shared, 3)
    n_rows = EP_SIZE * DP_SIZE * TOK_DEV
    x = jax.random.normal(key_tok, (n_rows, D_MODEL), jnp.float32).astype(jnp.bfloat16)
    gate = jax.random.uniform(key_gate, (n_rows, TOP_K), jnp.float32, 0.2, 0.8)
    w_gate = (jax.random.normal(key_wg, (EXPERTS, D_MODEL, FFN), jnp.float32) * D_MODEL ** -0.5).astype(jnp.bfloat16)
    w_up = (jax.random.normal(key_wu, (EXPERTS, D_MODEL, FFN), jnp.float32) * D_MODEL ** -0.5).astype(jnp.bfloat16)
    w_down = (jax.random.normal(key_wd, (EXPERTS, FFN, D_MODEL), jnp.float32) * (1.5 * FFN ** -0.5)).astype(jnp.bfloat16)
    return {"x": x, "expert_idx": route_ids(key_route), "gate": gate, "w_gate": w_gate, "w_up": w_up, "w_down": w_down}


def slot_table(ids_flat):
    one_hot = (ids_flat[:, None] == jnp.arange(EXPERTS, dtype=jnp.int32)[None, :]).astype(jnp.int32)
    slot_ids = jnp.sum((jnp.cumsum(one_hot, axis=0) - one_hot) * one_hot, axis=1)
    return jnp.where(slot_ids < CAPACITY, ids_flat * CAPACITY + slot_ids, EXPERTS * CAPACITY)


def take_rows(block, index):
    return jnp.take(block, index, axis=0, mode="fill", fill_value=0)


def reference(x, expert_idx, gate, w_gate, w_up, w_down):
    n_blocks = EP_SIZE * DP_SIZE
    x_blocks = x.reshape(n_blocks, TOK_DEV, D_MODEL)
    dest_row = jax.vmap(slot_table)(expert_idx.reshape(n_blocks, TOK_DEV * TOP_K))
    block_ids = jnp.arange(n_blocks)[:, None]
    pair_token = jnp.broadcast_to(jnp.arange(TOK_DEV * TOP_K, dtype=jnp.int32) // TOP_K, dest_row.shape)
    src_tok = jnp.full((n_blocks, EXPERTS * CAPACITY), TOK_DEV, jnp.int32).at[block_ids, dest_row].set(pair_token, mode="drop")
    slot_gate = jnp.zeros((n_blocks, EXPERTS * CAPACITY), jnp.float32).at[block_ids, dest_row].set(gate.reshape(n_blocks, TOK_DEV * TOP_K), mode="drop")
    src_by_exp = src_tok.reshape(n_blocks, EXPERTS, CAPACITY).transpose(1, 0, 2)
    gate_by_exp = slot_gate.reshape(n_blocks, EXPERTS, CAPACITY).transpose(1, 0, 2)

    def expert_step(running, inputs):
        src_e, gate_e, wg_e, wu_e, wd_e = inputs
        expert_rows = jax.vmap(take_rows)(x_blocks, src_e).reshape(n_blocks * CAPACITY, D_MODEL)
        gate_act = jnp.dot(expert_rows, wg_e, preferred_element_type=jnp.float32)
        up_act = jnp.dot(expert_rows, wu_e, preferred_element_type=jnp.float32)
        hidden = (jax.nn.silu(gate_act) * up_act).astype(jnp.bfloat16)
        out_rows = jnp.dot(hidden, wd_e, preferred_element_type=jnp.float32).astype(jnp.bfloat16)
        contrib = out_rows.reshape(n_blocks, CAPACITY, D_MODEL).astype(jnp.float32) * gate_e[:, :, None]
        return running.at[block_ids, src_e].add(contrib, mode="drop"), None

    summed = lax.scan(expert_step, x_blocks.astype(jnp.float32), (src_by_exp, gate_by_exp, w_gate, w_up, w_down))[0]
    return summed.astype(jnp.bfloat16).reshape(n_blocks * TOK_DEV, D_MODEL)
```

```python
import jax
import jax.numpy as jnp
from jax import lax
from jax.experimental import pallas as pl
from jax.experimental.pallas import tpu as pltpu
from jax.sharding import PartitionSpec as P

MESH = pl.DeviceIdType.MESH
F32 = jnp.float32
BF16 = jnp.bfloat16

T = 512
D = 2048
FF = 5632
FH = FF // 2
E = 8
C = 160
ROWS = 16 * C
FC = 256
NCH = FH // FC
MT = 640
NT = ROWS // MT
PAIR = range(2)
WA = 3072
WB = FF - WA
WBH = WB // 2
FIRST = 8
TICKS = NCH + 4


def al(v):
    return pl.multiple_of(v, 128)


def ynat(s, yl, o):
    return 2 * s + yl if o == 0 else 3 - (2 * s + yl)


def kernel(x_ref, idx_ref, gate_ref, wg_ref, wu_ref, wd_ref,
           y_ref, gu_ref, wdn_ref, back_ref,
           X, H, gv, dv, S, slot_ref, gw_ref,
           own_sem, ownsend_sem, loc_sem, nbr_recv, nbr_send, gu_recv, gu_send,
           wd0_recv, wd0_send, wd_recv, wd_send, tok_recv, tok_send, fwd_recv, fwd_send,
           h_recv, h_send, gl_sem, dl_sem, c_recv, c_send, bl_sem):
    p = lax.axis_index("expert")
    q = lax.axis_index("data")
    x = p // 2
    c = p % 2
    z = q // 4
    y = q % 4
    s = y // 2
    yl = y % 2
    e_own = 2 * x + s
    zm = (z + 3) % 4
    zp = (z + 1) % 4
    zo = (z + 2) % 4
    oc = dict(data=q, expert=2 * x + 1 - c)
    yp = dict(data=z * 4 + 2 * s + 1 - yl, expert=p)
    zpd = dict(data=zp * 4 + y, expert=p)
    zmd = dict(data=zm * 4 + y, expert=p)
    qc = z * 4 + 3 - y
    home = c == s
    b_own = 4 * x + c

    def remote(src, dst, ss, rs, dev):
        return pltpu.make_async_remote_copy(src_ref=src, dst_ref=dst, send_sem=ss, recv_sem=rs,
                                            device_id=dev, device_id_type=MESH)

    def half(i):
        return pl.ds(al(i * FH), FH)

    barrier = pltpu.get_barrier_semaphore()
    for dev in (yp, zpd, zmd):
        pl.semaphore_signal(barrier, inc=1, device_id=dev, device_id_type=MESH)

    def greet(b, _):
        od = (b // 2) % 2
        yd = od * (3 - y) + (1 - od) * y

        @pl.when(b != b_own)
        def _():
            pl.semaphore_signal(barrier, inc=1, device_id=dict(data=z * 4 + yd, expert=2 * (b // 4) + b % 2), device_id_type=MESH)
        return 0

    lax.fori_loop(0, 16, greet, 0)
    pl.semaphore_wait(barrier, 18)

    hx = pl.ds(al(c * FH), FH)
    my_rows = pl.ds(al((z * 4 + yl * 2) * 128), 128)

    def own_copy(m):
        src = (wg_ref, wu_ref)[m]
        return remote(src.at[0, :, half(1 - c)], gu_ref.at[m, my_rows, :], ownsend_sem.at[m], own_sem.at[m], oc)

    def bounce_in(m):
        src = (wg_ref, wu_ref)[m]
        return pltpu.make_async_copy(src.at[0, :, hx], H.at[pl.ds(m * 128, 128), hx], loc_sem.at[m])

    def bounce_out(m):
        return pltpu.make_async_copy(H.at[pl.ds(m * 128, 128), hx], gu_ref.at[m, my_rows, :], own_sem.at[m])

    def nbr_copy(f, h, m):
        src = (wg_ref, wu_ref)[m]
        cols = pl.ds(al(h * FH + f * FC), FC)
        dcols = pl.ds(al(f * FC), FC)
        nyl = (3 - y) % 2
        rows = pl.ds(al((z * 4 + nyl * 2 + 1) * 128), 128)
        return remote(src.at[0, :, cols], gu_ref.at[m, rows, dcols], nbr_send.at[f, h, m], nbr_recv.at[f, m],
                      dict(data=qc, expert=2 * x + h))

    def nbr_start(f):
        @pl.when(jnp.logical_not(home))
        def _():
            for h in PAIR:
                for m in PAIR:
                    nbr_copy(f, h, m).start()

    PARTS = ((WA, WB), (0, WA))

    def wd0_own(i):
        o, n = PARTS[i]
        return remote(wd_ref.at[0, pl.ds(o, n), :], wdn_ref.at[z, yl, pl.ds(o, n), :],
                      wd0_send.at[i], wd0_recv.at[i], oc)

    def wd0_nbr(i):
        o, n = PARTS[i]
        return remote(wd_ref.at[0, pl.ds(o, n), :], wdn_ref.at[z, (3 - y) % 2, pl.ds(o, n), :],
                      wd0_send.at[i], wd0_recv.at[i], dict(data=qc, expert=2 * x + 1))

    def wd0_loc(i):
        o, n = PARTS[i]
        return pltpu.make_async_copy(dv.at[0, pl.ds(o, n), pl.ds(0, 128)], wdn_ref.at[z, yl, pl.ds(o, n), :], wd0_recv.at[i])

    wd_in = pltpu.make_async_copy(wd_ref.at[0], dv.at[0, :, pl.ds(0, 128)], loc_sem.at[2])

    @pl.when(home)
    def _():
        for m in PAIR:
            own_copy(m).start()
            bounce_in(m).start()

        @pl.when(c == 0)
        def _():
            wd_in.start()

        for m in PAIR:
            bounce_in(m).wait()
            bounce_out(m).start()

        @pl.when(c == 0)
        def _():
            wd_in.wait()
            for i in PAIR:
                wd0_loc(i).start()

        @pl.when(c == 1)
        def _():
            for i in PAIR:
                wd0_own(i).start()

    for f in range(3):
        nbr_start(f)

    def rows(zz, l, o, n):
        return pl.ds(al((zz * 4 + l * 2 + o) * 128), n * 128)

    def guc(f, r, i, dev):
        ref = gu_ref.at[:, r, pl.ds(al(f * FC), FC)]
        return remote(ref, ref, gu_send.at[f, i], gu_recv.at[f, i], dev)

    SENT_A = ((z, yl, 0, 2, yp), (z, 0, 0, 4, zpd), (z, 0, 0, 4, zmd), (zm, 0, 0, 2, zpd), (zp, 1, 0, 2, zmd))
    GOT_A = ((z, 1 - yl, 0, 2), (zm, 0, 0, 4), (zp, 0, 0, 4), (zo, 0, 0, 2), (zo, 1, 0, 2))
    SENT_B = ((z, yl, 0, 2, zpd), (z, yl, 0, 2, zmd), (zm, yl, 0, 1, zpd), (zp, yl, 1, 1, zmd),
              (z, yl, 0, 2, yp), (zm, yl, 0, 2, yp), (zp, yl, 0, 2, yp), (zo, yl, 0, 2, yp))
    GOT_B = ((zm, yl, 0, 2), (zp, yl, 0, 2), (zo, yl, 0, 1), (zo, yl, 1, 1),
             (z, 1 - yl, 0, 2), (zm, 1 - yl, 0, 2), (zp, 1 - yl, 0, 2), (zo, 1 - yl, 0, 2))

    def gu_put(f, sent, *ids):
        for i in ids:
            guc(f, rows(*sent[i][:4]), i, sent[i][4]).start()

    def gu_got(f, table, *ids):
        for i in ids:
            guc(f, rows(*table[i]), i, yp).wait_recv()

    def by_tree(f, do_a, do_b):
        pl.when(f % 2 == 0)(do_a)
        pl.when(f % 2 == 1)(do_b)

    def stage1(f):
        for m in PAIR:
            nbr_copy(f, 0, m).wait_recv()

        def do_a():
            gu_put(f, SENT_A, 0)

        def do_b():
            gu_put(f, SENT_B, 0, 1, 4)

        by_tree(f, do_a, do_b)

    def stage2(f):
        def do_a():
            gu_got(f, GOT_A, 0)
            gu_put(f, SENT_A, 1, 2)

        def do_b():
            gu_got(f, GOT_B, 0)
            gu_put(f, SENT_B, 2, 5)
            gu_got(f, GOT_B, 1)
            gu_put(f, SENT_B, 3, 6)

        by_tree(f, do_a, do_b)

    def stage3(f):
        def do_a():
            gu_got(f, GOT_A, 1)
            gu_put(f, SENT_A, 3)
            gu_got(f, GOT_A, 2)
            gu_put(f, SENT_A, 4)

        def do_b():
            gu_got(f, GOT_B, 2, 3)
            gu_put(f, SENT_B, 7)

        by_tree(f, do_a, do_b)

    def stage4(f):
        def do_a():
            gu_got(f, GOT_A, 3, 4)

        def do_b():
            gu_got(f, GOT_B, 4, 5, 6, 7)

        by_tree(f, do_a, do_b)

    def guc_sends(f):
        def wait(sent):
            for i, t in enumerate(sent):
                guc(f, rows(*t[:4]), i, t[4]).wait_send()

        by_tree(f, lambda: wait(SENT_A), lambda: wait(SENT_B))

    def wdc(zz, l, o, n, i, dev):
        ref = wdn_ref.at[zz, l, pl.ds(o, n), :]
        return remote(ref, ref, wd_send.at[i], wd_recv.at[i], dev)

    A = (0, WA)
    B = (WA, WB)
    B0 = (WA, WBH)
    B1 = (WA + WBH, WBH)
    SENT = ((z, yl, *B, 0, zpd), (z, yl, *B, 1, zmd), (z, yl, *B, 2, yp),
            (z, yl, *A, 3, yp), (z, yl, *A, 4, zpd), (z, yl, *A, 5, zmd),
            (z, 1 - yl, *A, 6, zpd), (z, 1 - yl, *A, 7, zmd),
            (zm, yl, *B0, 8, zpd), (zp, yl, *B1, 9, zmd),
            (zm, yl, *B, 10, yp), (zp, yl, *B, 11, yp),
            (zm, 0, *A, 12, zpd), (zp, 1, *A, 13, zmd),
            (zo, yl, *B, 14, yp))
    GOT = ((zm, yl, *B, 0, zpd), (zp, yl, *B, 1, zmd), (z, 1 - yl, *B, 2, yp),
           (z, 1 - yl, *A, 3, yp), (zm, yl, *A, 4, zpd), (zp, yl, *A, 5, zmd),
           (zm, 1 - yl, *A, 6, zpd), (zp, 1 - yl, *A, 7, zmd),
           (zo, yl, *B0, 8, zpd), (zo, yl, *B1, 9, zmd),
           (zm, 1 - yl, *B, 10, yp), (zp, 1 - yl, *B, 11, yp),
           (zo, 0, *A, 12, zpd), (zo, 1, *A, 13, zmd),
           (zo, 1 - yl, *B, 14, yp))

    def put(*ids):
        for i in ids:
            wdc(*SENT[i]).start()

    def got(*ids):
        for i in ids:
            wdc(*GOT[i]).wait_recv()

    lanes = lax.broadcasted_iota(jnp.int32, (T, 128), 1)
    ids = jnp.transpose(idx_ref[...])
    gates = jnp.transpose(gate_ref[...])
    i0 = ids[:, 0:1]
    i1 = ids[:, 1:2]
    hit0 = i0 == lanes
    hit1 = i1 == lanes
    took = jnp.logical_or(hit0, hit1)
    took_f = jnp.where(took, 1.0, 0.0)
    lower = (lax.broadcasted_iota(jnp.int32, (T, T), 0) > lax.broadcasted_iota(jnp.int32, (T, T), 1))
    lower_f = jnp.where(lower, 1.0, 0.0).astype(BF16)
    count = jnp.dot(lower_f, took_f.astype(BF16), preferred_element_type=F32)
    slot_ref[...] = jnp.where(took, count, -1.0).astype(jnp.int32)
    gw_ref[...] = jnp.where(hit0, gates[:, 0:1], 0.0) + jnp.where(hit1, gates[:, 1:2], 0.0)

    def pick(e, r0, n):
        pos = lax.broadcasted_iota(jnp.int32, (n, C), 1)
        return jnp.where(slot_ref[pl.ds(r0, n), e:e + 1] == pos, 1.0, 0.0).astype(BF16)

    def tok_copy(e):
        xe, se = e // 2, e % 2
        same = jnp.where(s == se, 1, 0)
        yd = same * y + (1 - same) * (3 - y)
        o = 1 - same
        b = (x * 2 + o) * 2 + c
        return remote(S.at[e], X.at[pl.ds(pl.multiple_of(b * C, C), C), :],
                      tok_send.at[e], tok_recv.at[x * 2 + o], dict(data=z * 4 + yd, expert=2 * xe + c))

    for e in range(E):
        sel = pick(e, 0, T)
        for zz in range(4):
            r = lax.dot_general(sel, x_ref[:, zz * 512:(zz + 1) * 512], (((0,), (0,)), ((), ())),
                                preferred_element_type=F32).astype(BF16)
            for l in PAIR:
                for o in PAIR:
                    k = zz * 4 + l * 2 + o
                    n = ynat(e % 2, l, o)
                    S[e, :, k * 128:(k + 1) * 128] = r[:, n * 128:(n + 1) * 128]

    def mine(b):
        return pl.ds(pl.multiple_of(b * C, C), C)

    X[mine(b_own), :] = S[e_own]

    def fwd(j, k):
        ref = X.at[mine(j * 2 + k), :]
        return remote(ref, ref, fwd_send.at[j], fwd_recv.at[j], oc)

    def take_tokens(o):
        for j in range(o, 8, 2):
            @pl.when(j != x * 2)
            def _():
                pltpu.make_async_copy(S.at[0], X.at[mine(j * 2 + c), :], tok_recv.at[j]).wait()
            fwd(j, c).start()

    def gu_load(f):
        return pltpu.make_async_copy(gu_ref.at[:, :, pl.ds(al(f * FC), FC)], gv.at[f % 2], gl_sem.at[f % 2])

    def gu_compute(f):
        k = f % 2
        cols = pl.ds(al(c * FH + f * FC), FC)

        def tile(r, _):
            rr = pl.ds(pl.multiple_of(r * MT, MT), MT)
            g = jnp.dot(X[rr, :], gv[k, 0], preferred_element_type=F32)
            u = jnp.dot(X[rr, :], gv[k, 1], preferred_element_type=F32)
            H[rr, cols] = (jax.nn.silu(g) * u).astype(BF16)
            return 0

        lax.fori_loop(0, NT, tile, 0)

    def h_copy(f, k):
        ref = H.at[:, pl.ds(al(k * FH + f * FC), FC)]
        return remote(ref, ref, h_send.at[f], h_recv.at[f], oc)

    def one_chunk(j):
        @pl.when(jnp.logical_or(j == 0, j >= FIRST))
        def _():
            gu_load(j).start()

        @pl.when(j + 1 < FIRST)
        def _():
            gu_load(j + 1).start()

        gu_load(j).wait()
        gu_compute(j)

        @pl.when(j > 0)
        def _():
            h_copy(j - 1, c).start()

    def done_by(i):
        return jnp.where(i < FIRST, 0, jnp.minimum(2 * (i - FIRST + 1), i - 3))

    def during(i, lo, hi, fn):
        pl.when(jnp.logical_and(i >= lo, i < hi))(fn)

    def tick(i, _):
        @pl.when(i == 0)
        def _():
            for m in PAIR:
                own_copy(m).wait_recv()

        during(i, 0, NCH, lambda: stage1(i))
        during(i, 0, E - 1, lambda: tok_copy((e_own + 1 + i) % E).start())
        during(i, 0, NCH - 3, lambda: nbr_start(i + 3))

        @pl.when(jnp.logical_and(i == NCH - 3, jnp.logical_not(home)))
        def _():
            for k in PAIR:
                wd0_nbr(k).start()

        during(i, 2, NCH + 2, lambda: stage3(i - 2))
        during(i, 1, NCH + 1, lambda: stage2(i - 1))

        @pl.when(i == NCH)
        def _():
            wd0_nbr(0).wait_recv()
            put(0, 1, 2)

        @pl.when(i == NCH + 1)
        def _():
            wd0_nbr(1).wait_recv()
            put(3, 4, 5)

        @pl.when(i == NCH + 2)
        def _():
            got(0)
            put(8, 10)
            got(1)
            put(9, 11)

        @pl.when(i == NCH + 3)
        def _():
            got(3)
            put(6, 7)

        during(i, 4, NCH + 4, lambda: stage4(i - 4))

        @pl.when(i == FIRST - 3)
        def _():
            take_tokens(0)

        @pl.when(i == FIRST)
        def _():
            take_tokens(1)
            for j in range(8):
                fwd(j, 1 - c).wait_recv()

        def chunk(j, _):
            one_chunk(j)
            return 0

        lax.fori_loop(done_by(i - 1), done_by(i), chunk, 0)
        return 0

    lax.fori_loop(0, TICKS, tick, 0)
    h_copy(NCH - 1, c).start()

    def d_load(g, zz):
        out = []
        for l in PAIR:
            lane = pl.ds(al(((l + c) % 2) * 128), 128)
            out.append(pltpu.make_async_copy(wdn_ref.at[zz, l], dv.at[g % 2, :, lane], dl_sem.at[g % 2, l]))
        return out

    def place(zz):
        w = c * (1 - s) + (1 - c) * s
        return pl.ds(al(zz * 512 + w * 256), 256)

    def out_copy(g, zz, b):
        xd = b // 4
        cd = b % 2
        od = (b // 2) % 2
        yd = od * (3 - y) + (1 - od) * y
        return remote(X.at[mine(b), pl.ds(g * 256, 256)], back_ref.at[e_own, :, place(zz)],
                      c_send.at[g], c_recv.at[g], dict(data=z * 4 + yd, expert=2 * xd + cd))

    def out_send(g, zz, r):
        for k in range(4):
            b = r * 4 + k

            @pl.when(b != b_own)
            def _():
                out_copy(g, zz, b).start()

    def out_compute(g, zz):
        for d in d_load(g, zz):
            d.wait()

        def tile(r, _):
            rr = pl.ds(pl.multiple_of(r * MT, MT), MT)
            X[rr, g * 256:(g + 1) * 256] = jnp.dot(H[rr, :], dv[g % 2], preferred_element_type=F32).astype(BF16)

            @pl.when(r > 0)
            def _():
                out_send(g, zz, r - 1)
            return 0

        lax.fori_loop(0, NT, tile, 0)
        out_send(g, zz, NT - 1)
        pltpu.make_async_copy(X.at[mine(b_own), pl.ds(g * 256, 256)], back_ref.at[e_own, :, place(zz)], c_recv.at[g]).start()

    def got_all(g):
        pltpu.make_async_copy(X.at[:, pl.ds(0, 256)], X.at[:, pl.ds(0, 256)], c_recv.at[g]).wait()

    def sent_all(g):
        pltpu.make_async_copy(X.at[pl.ds(0, 15 * C), pl.ds(0, 256)], X.at[pl.ds(0, 15 * C), pl.ds(0, 256)], c_send.at[g]).wait()

    def finish(g, zz):
        got_all(g)
        cols = pl.ds(al(zz * 512), 512)
        back = pltpu.make_async_copy(back_ref.at[:, :, cols], S.at[:, :, cols], bl_sem.at[0])
        back.start()
        back.wait()

        def tile(t, _):
            rr = pl.ds(pl.multiple_of(t * 256, 256), 256)
            acc = x_ref[rr, cols].astype(F32)
            for e in range(E):
                part = jnp.dot(pick(e, pl.multiple_of(t * 256, 256), 256), S[e, :, cols], preferred_element_type=F32)
                acc = acc + gw_ref[rr, e:e + 1] * part
            y_ref[rr, cols] = acc.astype(BF16)
            return 0

        lax.fori_loop(0, 2, tile, 0)

    for j in range(8):
        fwd(j, c).wait_send()
    for e in range(E):
        @pl.when(e != e_own)
        def _():
            tok_copy(e).wait_send()

    got(2)
    for d in d_load(0, z):
        d.start()
    for f in range(NCH):
        h_copy(f, 1 - c).wait_recv()
    out_compute(0, z)
    got(8, 9)
    put(14)
    got(4, 5, 6, 7)
    put(12, 13)
    got(10)
    for d in d_load(1, zm):
        d.start()
    got(11)
    out_compute(1, zm)
    for d in d_load(2, zp):
        d.start()
    out_compute(2, zp)
    finish(0, z)
    got(12, 13, 14)
    for d in d_load(3, zo):
        d.start()
    out_compute(3, zo)
    finish(1, zm)
    finish(2, zp)
    finish(3, zo)

    def drain(f, _):
        guc_sends(f)
        h_copy(f, c).wait_send()

        @pl.when(jnp.logical_not(home))
        def _():
            for h in PAIR:
                for m in PAIR:
                    nbr_copy(f, h, m).wait_send()
        return 0

    lax.fori_loop(0, NCH, drain, 0)
    for i in range(15):
        wdc(*SENT[i]).wait_send()
    for g in range(4):
        sent_all(g)

    @pl.when(home)
    def _():
        for m in PAIR:
            own_copy(m).wait_send()

    @pl.when(jnp.logical_or(jnp.logical_not(home), c == 1))
    def _():
        for i in PAIR:
            wd0_nbr(i).wait_send()


def solution(mesh):
    tok_spec = P(("rep", "expert", "data"), None)
    wide_spec = P("expert", "data", None)
    down_spec = P("expert", None, "data")
    dma = pltpu.SemaphoreType.DMA
    two, four, eight = dma((2,)), dma((4,)), dma((E,))
    hbm = pl.BlockSpec(memory_space=pltpu.HBM)
    vmem = pl.BlockSpec(memory_space=pltpu.VMEM)

    def device_step(x_loc, idx_loc, gate_loc, wg_loc, wu_loc, wd_loc):
        out = pl.pallas_call(
            kernel,
            out_shape=(jax.ShapeDtypeStruct((T, D), BF16),
                       jax.ShapeDtypeStruct((2, D, FH), BF16),
                       jax.ShapeDtypeStruct((4, 2, FF, 128), BF16),
                       jax.ShapeDtypeStruct((E, C, D), BF16)),
            in_specs=[vmem, vmem, vmem, hbm, hbm, hbm],
            out_specs=(vmem, hbm, hbm, hbm),
            scratch_shapes=[
                pltpu.VMEM((ROWS, D), BF16),
                pltpu.VMEM((ROWS, FF), BF16),
                pltpu.VMEM((2, 2, D, FC), BF16),
                pltpu.VMEM((2, FF, 256), BF16),
                pltpu.VMEM((E, C, D), BF16),
                pltpu.VMEM((T, 128), jnp.int32),
                pltpu.VMEM((T, 128), F32),
                two, two, dma((3,)),
                dma((NCH, 2)), dma((NCH, 2, 2)),
                dma((NCH, E)), dma((NCH, E)),
                two, two, dma((15,)), dma((15,)),
                eight, eight, eight, eight,
                dma((NCH,)), dma((NCH,)), two, dma((2, 2)),
                four, four, dma((1,)),
            ],
            compiler_params=pltpu.CompilerParams(has_side_effects=True, collective_id=0, vmem_limit_bytes=67043328),
        )(x_loc, idx_loc.T, gate_loc.T, wg_loc, wu_loc, wd_loc)
        return out[0]

    return jax.shard_map(device_step, mesh=mesh, in_specs=(tok_spec, tok_spec, tok_spec, wide_spec, wide_spec, down_spec), out_specs=tok_spec, check_vma=False)
```

```python
import jax
import jax.numpy as jnp
from jax import lax
from jax.experimental import pallas as pl
from jax.experimental.pallas import tpu as pltpu
from jax.sharding import PartitionSpec as P

MESH = pl.DeviceIdType.MESH
F32 = jnp.float32
BF16 = jnp.bfloat16

T = 512
D = 2048
FF = 5632
FH = FF // 2
E = 8
C = 160
ROWS = 16 * C
FC = 256
NCH = FH // FC
MT = 640
NT = ROWS // MT
PAIR = range(2)
WA = 3072
WB = FF - WA
WBH = WB // 2
FIRST = 8
TICKS = NCH + 4


def al(v):
    return pl.multiple_of(v, 128)


def ynat(s, yl, o):
    return 2 * s + yl if o == 0 else 3 - (2 * s + yl)


def kernel(x_ref, idx_ref, gate_ref, wg_ref, wu_ref, wd_ref,
           y_ref, gu_ref, wdn_ref, back_ref,
           X, H, gv, dv, S, slot_ref, gw_ref,
           own_sem, ownsend_sem, loc_sem, nbr_recv, nbr_send, gu_recv, gu_send,
           wd0_recv, wd0_send, wd_recv, wd_send, tok_recv, tok_send, fwd_recv, fwd_send,
           h_recv, h_send, gl_sem, dl_sem, c_recv, c_send, bl_sem):
    p = lax.axis_index("expert")
    q = lax.axis_index("data")
    x = p // 2
    c = p % 2
    z = q // 4
    y = q % 4
    s = y // 2
    yl = y % 2
    e_own = 2 * x + s
    zm = (z + 3) % 4
    zp = (z + 1) % 4
    zo = (z + 2) % 4
    oc = dict(data=q, expert=2 * x + 1 - c)
    yp = dict(data=z * 4 + 2 * s + 1 - yl, expert=p)
    zpd = dict(data=zp * 4 + y, expert=p)
    zmd = dict(data=zm * 4 + y, expert=p)
    qc = z * 4 + 3 - y
    home = c == s
    b_own = 4 * x + c

    def remote(src, dst, ss, rs, dev):
        return pltpu.make_async_remote_copy(src_ref=src, dst_ref=dst, send_sem=ss, recv_sem=rs,
                                            device_id=dev, device_id_type=MESH)

    def half(i):
        return pl.ds(al(i * FH), FH)

    barrier = pltpu.get_barrier_semaphore()
    for dev in (yp, zpd, zmd):
        pl.semaphore_signal(barrier, inc=1, device_id=dev, device_id_type=MESH)

    def greet(b, _):
        od = (b // 2) % 2
        yd = od * (3 - y) + (1 - od) * y

        @pl.when(b != b_own)
        def _():
            pl.semaphore_signal(barrier, inc=1, device_id=dict(data=z * 4 + yd, expert=2 * (b // 4) + b % 2), device_id_type=MESH)
        return 0

    lax.fori_loop(0, 16, greet, 0)
    pl.semaphore_wait(barrier, 18)

    hx = pl.ds(al(c * FH), FH)
    my_rows = pl.ds(al((z * 4 + yl * 2) * 128), 128)

    def own_copy(m):
        src = (wg_ref, wu_ref)[m]
        return remote(src.at[0, :, half(1 - c)], gu_ref.at[m, my_rows, :], ownsend_sem.at[m], own_sem.at[m], oc)

    def bounce_in(m):
        src = (wg_ref, wu_ref)[m]
        return pltpu.make_async_copy(src.at[0, :, hx], H.at[pl.ds(m * 128, 128), hx], loc_sem.at[m])

    def bounce_out(m):
        return pltpu.make_async_copy(H.at[pl.ds(m * 128, 128), hx], gu_ref.at[m, my_rows, :], own_sem.at[m])

    def nbr_copy(f, h, m):
        src = (wg_ref, wu_ref)[m]
        cols = pl.ds(al(h * FH + f * FC), FC)
        dcols = pl.ds(al(f * FC), FC)
        nyl = (3 - y) % 2
        rows = pl.ds(al((z * 4 + nyl * 2 + 1) * 128), 128)
        return remote(src.at[0, :, cols], gu_ref.at[m, rows, dcols], nbr_send.at[f, h, m], nbr_recv.at[f, m],
                      dict(data=qc, expert=2 * x + h))

    def nbr_start(f):
        @pl.when(jnp.logical_not(home))
        def _():
            for h in PAIR:
                for m in PAIR:
                    nbr_copy(f, h, m).start()

    PARTS = ((WA, WB), (0, WA))

    def wd0_own(i):
        o, n = PARTS[i]
        return remote(wd_ref.at[0, pl.ds(o, n), :], wdn_ref.at[z, yl, pl.ds(o, n), :],
                      wd0_send.at[i], wd0_recv.at[i], oc)

    def wd0_nbr(i):
        o, n = PARTS[i]
        return remote(wd_ref.at[0, pl.ds(o, n), :], wdn_ref.at[z, (3 - y) % 2, pl.ds(o, n), :],
                      wd0_send.at[i], wd0_recv.at[i], dict(data=qc, expert=2 * x + 1))

    def wd0_loc(i):
        o, n = PARTS[i]
        return pltpu.make_async_copy(dv.at[0, pl.ds(o, n), pl.ds(0, 128)], wdn_ref.at[z, yl, pl.ds(o, n), :], wd0_recv.at[i])

    wd_in = pltpu.make_async_copy(wd_ref.at[0], dv.at[0, :, pl.ds(0, 128)], loc_sem.at[2])

    @pl.when(home)
    def _():
        for m in PAIR:
            own_copy(m).start()
            bounce_in(m).start()

        @pl.when(c == 0)
        def _():
            wd_in.start()

        for m in PAIR:
            bounce_in(m).wait()
            bounce_out(m).start()

        @pl.when(c == 0)
        def _():
            wd_in.wait()
            for i in PAIR:
                wd0_loc(i).start()

        @pl.when(c == 1)
        def _():
            for i in PAIR:
                wd0_own(i).start()

    for f in range(3):
        nbr_start(f)

    def rows(zz, l, o, n):
        return pl.ds(al((zz * 4 + l * 2 + o) * 128), n * 128)

    def guc(f, r, i, dev):
        ref = gu_ref.at[:, r, pl.ds(al(f * FC), FC)]
        return remote(ref, ref, gu_send.at[f, i], gu_recv.at[f, i], dev)

    SENT_A = ((z, yl, 0, 2, yp), (z, 0, 0, 4, zpd), (z, 0, 0, 4, zmd), (zm, 0, 0, 2, zpd), (zp, 1, 0, 2, zmd))
    GOT_A = ((z, 1 - yl, 0, 2), (zm, 0, 0, 4), (zp, 0, 0, 4), (zo, 0, 0, 2), (zo, 1, 0, 2))
    SENT_B = ((z, yl, 0, 2, zpd), (z, yl, 0, 2, zmd), (zm, yl, 0, 1, zpd), (zp, yl, 1, 1, zmd),
              (z, yl, 0, 2, yp), (zm, yl, 0, 2, yp), (zp, yl, 0, 2, yp), (zo, yl, 0, 2, yp))
    GOT_B = ((zm, yl, 0, 2), (zp, yl, 0, 2), (zo, yl, 0, 1), (zo, yl, 1, 1),
             (z, 1 - yl, 0, 2), (zm, 1 - yl, 0, 2), (zp, 1 - yl, 0, 2), (zo, 1 - yl, 0, 2))

    def gu_put(f, sent, *ids):
        for i in ids:
            guc(f, rows(*sent[i][:4]), i, sent[i][4]).start()

    def gu_got(f, table, *ids):
        for i in ids:
            guc(f, rows(*table[i]), i, yp).wait_recv()

    def by_tree(f, do_a, do_b):
        pl.when(f % 2 == 0)(do_a)
        pl.when(f % 2 == 1)(do_b)

    def stage1(f):
        for m in PAIR:
            nbr_copy(f, 0, m).wait_recv()

        def do_a():
            gu_put(f, SENT_A, 0)

        def do_b():
            gu_put(f, SENT_B, 0, 1, 4)

        by_tree(f, do_a, do_b)

    def stage2(f):
        def do_a():
            gu_got(f, GOT_A, 0)
            gu_put(f, SENT_A, 1, 2)

        def do_b():
            gu_got(f, GOT_B, 0)
            gu_put(f, SENT_B, 2, 5)
            gu_got(f, GOT_B, 1)
            gu_put(f, SENT_B, 3, 6)

        by_tree(f, do_a, do_b)

    def stage3(f):
        def do_a():
            gu_got(f, GOT_A, 1)
            gu_put(f, SENT_A, 3)
            gu_got(f, GOT_A, 2)
            gu_put(f, SENT_A, 4)

        def do_b():
            gu_got(f, GOT_B, 2, 3)
            gu_put(f, SENT_B, 7)

        by_tree(f, do_a, do_b)

    def stage4(f):
        def do_a():
            gu_got(f, GOT_A, 3, 4)

        def do_b():
            gu_got(f, GOT_B, 4, 5, 6, 7)

        by_tree(f, do_a, do_b)

    def guc_sends(f):
        def wait(sent):
            for i, t in enumerate(sent):
                guc(f, rows(*t[:4]), i, t[4]).wait_send()

        by_tree(f, lambda: wait(SENT_A), lambda: wait(SENT_B))

    def wdc(zz, l, o, n, i, dev):
        ref = wdn_ref.at[zz, l, pl.ds(o, n), :]
        return remote(ref, ref, wd_send.at[i], wd_recv.at[i], dev)

    A = (0, WA)
    B = (WA, WB)
    B0 = (WA, WBH)
    B1 = (WA + WBH, WBH)
    SENT = ((z, yl, *B, 0, zpd), (z, yl, *B, 1, zmd), (z, yl, *B, 2, yp),
            (z, yl, *A, 3, yp), (z, yl, *A, 4, zpd), (z, yl, *A, 5, zmd),
            (z, 1 - yl, *A, 6, zpd), (z, 1 - yl, *A, 7, zmd),
            (zm, yl, *B0, 8, zpd), (zp, yl, *B1, 9, zmd),
            (zm, yl, *B, 10, yp), (zp, yl, *B, 11, yp),
            (zm, 0, *A, 12, zpd), (zp, 1, *A, 13, zmd),
            (zo, yl, *B, 14, yp))
    GOT = ((zm, yl, *B, 0, zpd), (zp, yl, *B, 1, zmd), (z, 1 - yl, *B, 2, yp),
           (z, 1 - yl, *A, 3, yp), (zm, yl, *A, 4, zpd), (zp, yl, *A, 5, zmd),
           (zm, 1 - yl, *A, 6, zpd), (zp, 1 - yl, *A, 7, zmd),
           (zo, yl, *B0, 8, zpd), (zo, yl, *B1, 9, zmd),
           (zm, 1 - yl, *B, 10, yp), (zp, 1 - yl, *B, 11, yp),
           (zo, 0, *A, 12, zpd), (zo, 1, *A, 13, zmd),
           (zo, 1 - yl, *B, 14, yp))

    def put(*ids):
        for i in ids:
            wdc(*SENT[i]).start()

    def got(*ids):
        for i in ids:
            wdc(*GOT[i]).wait_recv()

    lanes = lax.broadcasted_iota(jnp.int32, (T, 128), 1)
    ids = jnp.transpose(idx_ref[...])
    gates = jnp.transpose(gate_ref[...])
    i0 = ids[:, 0:1]
    i1 = ids[:, 1:2]
    hit0 = i0 == lanes
    hit1 = i1 == lanes
    took = jnp.logical_or(hit0, hit1)
    took_f = jnp.where(took, 1.0, 0.0)
    lower = (lax.broadcasted_iota(jnp.int32, (T, T), 0) > lax.broadcasted_iota(jnp.int32, (T, T), 1))
    lower_f = jnp.where(lower, 1.0, 0.0).astype(BF16)
    count = jnp.dot(lower_f, took_f.astype(BF16), preferred_element_type=F32)
    slot_ref[...] = jnp.where(took, count, -1.0).astype(jnp.int32)
    gw_ref[...] = jnp.where(hit0, gates[:, 0:1], 0.0) + jnp.where(hit1, gates[:, 1:2], 0.0)

    def pick(e, r0, n):
        pos = lax.broadcasted_iota(jnp.int32, (n, C), 1)
        return jnp.where(slot_ref[pl.ds(r0, n), e:e + 1] == pos, 1.0, 0.0).astype(BF16)

    def tok_copy(e):
        xe, se = e // 2, e % 2
        same = jnp.where(s == se, 1, 0)
        yd = same * y + (1 - same) * (3 - y)
        o = 1 - same
        b = (x * 2 + o) * 2 + c
        return remote(S.at[e], X.at[pl.ds(pl.multiple_of(b * C, C), C), :],
                      tok_send.at[e], tok_recv.at[x * 2 + o], dict(data=z * 4 + yd, expert=2 * xe + c))

    for e in range(E):
        sel = pick(e, 0, T)
        for zz in range(4):
            r = lax.dot_general(sel, x_ref[:, zz * 512:(zz + 1) * 512], (((0,), (0,)), ((), ())),
                                preferred_element_type=F32).astype(BF16)
            for l in PAIR:
                for o in PAIR:
                    k = zz * 4 + l * 2 + o
                    n = ynat(e % 2, l, o)
                    S[e, :, k * 128:(k + 1) * 128] = r[:, n * 128:(n + 1) * 128]
        if e == 0:
            for m in PAIR:
                own_copy(m).wait_recv()
            stage1(0)
            nbr_start(3)
        if e == 3:
            stage1(1)
        if e == 6:
            stage2(0)
            nbr_start(4)

    def mine(b):
        return pl.ds(pl.multiple_of(b * C, C), C)

    X[mine(b_own), :] = S[e_own]

    def fwd(j, k):
        ref = X.at[mine(j * 2 + k), :]
        return remote(ref, ref, fwd_send.at[j], fwd_recv.at[j], oc)

    def take_tokens(o):
        for j in range(o, 8, 2):
            @pl.when(j != x * 2)
            def _():
                pltpu.make_async_copy(S.at[0], X.at[mine(j * 2 + c), :], tok_recv.at[j]).wait()
            fwd(j, c).start()

    def gu_load(f):
        return pltpu.make_async_copy(gu_ref.at[:, :, pl.ds(al(f * FC), FC)], gv.at[f % 2], gl_sem.at[f % 2])

    def gu_compute(f):
        k = f % 2
        cols = pl.ds(al(c * FH + f * FC), FC)

        def tile(r, _):
            rr = pl.ds(pl.multiple_of(r * MT, MT), MT)
            g = jnp.dot(X[rr, :], gv[k, 0], preferred_element_type=F32)
            u = jnp.dot(X[rr, :], gv[k, 1], preferred_element_type=F32)
            H[rr, cols] = (jax.nn.silu(g) * u).astype(BF16)
            return 0

        lax.fori_loop(0, NT, tile, 0)

    def h_copy(f, k):
        ref = H.at[:, pl.ds(al(k * FH + f * FC), FC)]
        return remote(ref, ref, h_send.at[f], h_recv.at[f], oc)

    def one_chunk(j):
        @pl.when(jnp.logical_or(j == 0, j >= FIRST))
        def _():
            gu_load(j).start()

        @pl.when(j + 1 < FIRST)
        def _():
            gu_load(j + 1).start()

        gu_load(j).wait()
        gu_compute(j)

        @pl.when(j > 0)
        def _():
            h_copy(j - 1, c).start()

    def done_by(i):
        return jnp.where(i < FIRST, 0, jnp.minimum(2 * (i - FIRST + 1), i - 3))

    def during(i, lo, hi, fn):
        pl.when(jnp.logical_and(i >= lo, i < hi))(fn)

    def tick(i, _):
        during(i, 2, NCH, lambda: stage1(i))
        during(i, 2, NCH - 3, lambda: nbr_start(i + 3))

        @pl.when(jnp.logical_and(i == NCH - 3, jnp.logical_not(home)))
        def _():
            for k in PAIR:
                wd0_nbr(k).start()

        during(i, 2, NCH + 1, lambda: stage2(i - 1))
        during(i, 2, E - 1, lambda: tok_copy((e_own + 1 + i) % E).start())

        @pl.when(i == NCH - 1)
        def _():
            wd0_nbr(0).wait_recv()
            put(0, 1, 2)

        @pl.when(i == NCH)
        def _():
            wd0_nbr(1).wait_recv()
            put(3, 4, 5)

        @pl.when(i == NCH + 1)
        def _():
            got(0)
            put(8, 10)
            got(1)
            put(9, 11)

        @pl.when(i == NCH + 2)
        def _():
            got(3)
            put(6, 7)

        during(i, 4, NCH + 4, lambda: stage4(i - 4))

        @pl.when(i == FIRST - 1)
        def _():
            take_tokens(0)

        @pl.when(i == FIRST)
        def _():
            take_tokens(1)
            for j in range(8):
                fwd(j, 1 - c).wait_recv()

        def chunk(j, _):
            one_chunk(j)
            return 0

        mid = jnp.minimum(done_by(i - 1) + 1, done_by(i))
        lax.fori_loop(done_by(i - 1), mid, chunk, 0)
        during(i, 2, NCH + 2, lambda: stage3(i - 2))
        lax.fori_loop(mid, done_by(i), chunk, 0)
        return 0

    tok_copy((e_own + 1) % E).start()
    tok_copy((e_own + 2) % E).start()
    lax.fori_loop(2, TICKS, tick, 0)
    h_copy(NCH - 1, c).start()

    def d_load(g, zz):
        out = []
        for l in PAIR:
            lane = pl.ds(al(((l + c) % 2) * 128), 128)
            out.append(pltpu.make_async_copy(wdn_ref.at[zz, l], dv.at[g % 2, :, lane], dl_sem.at[g % 2, l]))
        return out

    def place(zz):
        w = c * (1 - s) + (1 - c) * s
        return pl.ds(al(zz * 512 + w * 256), 256)

    def out_copy(g, zz, b):
        xd = b // 4
        cd = b % 2
        od = (b // 2) % 2
        yd = od * (3 - y) + (1 - od) * y
        return remote(X.at[mine(b), pl.ds(g * 256, 256)], back_ref.at[e_own, :, place(zz)],
                      c_send.at[g], c_recv.at[g], dict(data=z * 4 + yd, expert=2 * xd + cd))

    def out_send(g, zz, r):
        for k in range(4):
            b = r * 4 + k

            @pl.when(b != b_own)
            def _():
                out_copy(g, zz, b).start()

    def out_compute(g, zz):
        for d in d_load(g, zz):
            d.wait()

        def turn(k):
            return (x + 1 + k) % NT

        def tile(k, _):
            rr = pl.ds(pl.multiple_of(turn(k) * MT, MT), MT)
            X[rr, g * 256:(g + 1) * 256] = jnp.dot(H[rr, :], dv[g % 2], preferred_element_type=F32).astype(BF16)

            @pl.when(k > 0)
            def _():
                out_send(g, zz, turn(k - 1))
            return 0

        lax.fori_loop(0, NT, tile, 0)
        out_send(g, zz, turn(NT - 1))
        pltpu.make_async_copy(X.at[mine(b_own), pl.ds(g * 256, 256)], back_ref.at[e_own, :, place(zz)], c_recv.at[g]).start()

    def got_all(g):
        pltpu.make_async_copy(X.at[:, pl.ds(0, 256)], X.at[:, pl.ds(0, 256)], c_recv.at[g]).wait()

    def sent_all(g):
        pltpu.make_async_copy(X.at[pl.ds(0, 15 * C), pl.ds(0, 256)], X.at[pl.ds(0, 15 * C), pl.ds(0, 256)], c_send.at[g]).wait()

    def finish(g, zz):
        got_all(g)
        cols = pl.ds(al(zz * 512), 512)
        back = pltpu.make_async_copy(back_ref.at[:, :, cols], S.at[:, :, cols], bl_sem.at[0])
        back.start()
        back.wait()

        def tile(t, _):
            rr = pl.ds(pl.multiple_of(t * 256, 256), 256)
            acc = x_ref[rr, cols].astype(F32)
            for e in range(E):
                part = jnp.dot(pick(e, pl.multiple_of(t * 256, 256), 256), S[e, :, cols], preferred_element_type=F32)
                acc = acc + gw_ref[rr, e:e + 1] * part
            y_ref[rr, cols] = acc.astype(BF16)
            return 0

        lax.fori_loop(0, 2, tile, 0)

    for j in range(8):
        fwd(j, c).wait_send()
    for e in range(E):
        @pl.when(e != e_own)
        def _():
            tok_copy(e).wait_send()

    got(2)
    for d in d_load(0, z):
        d.start()
    for f in range(NCH):
        h_copy(f, 1 - c).wait_recv()
    out_compute(0, z)
    got(8, 9)
    put(14)
    got(4, 5, 6, 7)
    put(12, 13)
    got(10)
    for d in d_load(1, zm):
        d.start()
    got(11)
    out_compute(1, zm)
    for d in d_load(2, zp):
        d.start()
    out_compute(2, zp)
    finish(0, z)
    got(12, 13, 14)
    for d in d_load(3, zo):
        d.start()
    out_compute(3, zo)
    finish(1, zm)
    finish(2, zp)
    finish(3, zo)

    def drain(f, _):
        guc_sends(f)
        h_copy(f, c).wait_send()

        @pl.when(jnp.logical_not(home))
        def _():
            for h in PAIR:
                for m in PAIR:
                    nbr_copy(f, h, m).wait_send()
        return 0

    lax.fori_loop(0, NCH, drain, 0)
    for i in range(15):
        wdc(*SENT[i]).wait_send()
    for g in range(4):
        sent_all(g)

    @pl.when(home)
    def _():
        for m in PAIR:
            own_copy(m).wait_send()

    @pl.when(jnp.logical_or(jnp.logical_not(home), c == 1))
    def _():
        for i in PAIR:
            wd0_nbr(i).wait_send()


def solution(mesh):
    tok_spec = P(("rep", "expert", "data"), None)
    wide_spec = P("expert", "data", None)
    down_spec = P("expert", None, "data")
    dma = pltpu.SemaphoreType.DMA
    two, four, eight = dma((2,)), dma((4,)), dma((E,))
    hbm = pl.BlockSpec(memory_space=pltpu.HBM)
    vmem = pl.BlockSpec(memory_space=pltpu.VMEM)

    def device_step(x_loc, idx_loc, gate_loc, wg_loc, wu_loc, wd_loc):
        out = pl.pallas_call(
            kernel,
            out_shape=(jax.ShapeDtypeStruct((T, D), BF16),
                       jax.ShapeDtypeStruct((2, D, FH), BF16),
                       jax.ShapeDtypeStruct((4, 2, FF, 128), BF16),
                       jax.ShapeDtypeStruct((E, C, D), BF16)),
            in_specs=[vmem, vmem, vmem, hbm, hbm, hbm],
            out_specs=(vmem, hbm, hbm, hbm),
            scratch_shapes=[
                pltpu.VMEM((ROWS, D), BF16),
                pltpu.VMEM((ROWS, FF), BF16),
                pltpu.VMEM((2, 2, D, FC), BF16),
                pltpu.VMEM((2, FF, 256), BF16),
                pltpu.VMEM((E, C, D), BF16),
                pltpu.VMEM((T, 128), jnp.int32),
                pltpu.VMEM((T, 128), F32),
                two, two, dma((3,)),
                dma((NCH, 2)), dma((NCH, 2, 2)),
                dma((NCH, E)), dma((NCH, E)),
                two, two, dma((15,)), dma((15,)),
                eight, eight, eight, eight,
                dma((NCH,)), dma((NCH,)), two, dma((2, 2)),
                four, four, dma((1,)),
            ],
            compiler_params=pltpu.CompilerParams(has_side_effects=True, collective_id=0, vmem_limit_bytes=67043328),
        )(x_loc, idx_loc.T, gate_loc.T, wg_loc, wu_loc, wd_loc)
        return out[0]

    return jax.shard_map(device_step, mesh=mesh, in_specs=(tok_spec, tok_spec, tok_spec, wide_spec, wide_spec, down_spec), out_specs=tok_spec, check_vma=False)
```

```python
import jax
import jax.numpy as jnp
from jax import lax
from jax.experimental import pallas as pl
from jax.experimental.pallas import tpu as pltpu
from jax.sharding import PartitionSpec as P

MESH = pl.DeviceIdType.MESH
F32 = jnp.float32
BF16 = jnp.bfloat16

T = 512
D = 2048
FF = 5632
FH = FF // 2
E = 8
C = 160
ROWS = 16 * C
FC = 256
NCH = FH // FC
MT = 640
NT = ROWS // MT
PAIR = range(2)
WA = 3072
WB = FF - WA
WBH = WB // 2
FIRST = 8
TICKS = NCH + 4


L = 128


def al(v):
    return pl.multiple_of(v, L)


def ynat(s, yl, o):
    return 2 * s + yl if o == 0 else 3 - (2 * s + yl)


def kernel(x_ref, idx_ref, gate_ref, wg_ref, wu_ref, wd_ref,
           y_ref, gu_ref, wdn_ref, back_ref,
           X, H, gv, dv, S, slot_ref, gw_ref,
           own_sem, ownsend_sem, loc_sem, nbr_recv, nbr_send, gu_recv, gu_send,
           wd0_recv, wd0_send, wd_recv, wd_send, tok_recv, tok_send, fwd_recv, fwd_send,
           h_recv, h_send, gl_sem, dl_sem, c_recv, c_send, bl_sem):
    p = lax.axis_index("expert")
    q = lax.axis_index("data")
    x = p // 2
    c = p % 2
    z = q // 4
    y = q % 4
    s = y // 2
    yl = y % 2
    e_own = 2 * x + s
    zm = (z + 3) % 4
    zp = (z + 1) % 4
    zo = (z + 2) % 4
    oc = dict(data=q, expert=2 * x + 1 - c)
    yp = dict(data=z * 4 + 2 * s + 1 - yl, expert=p)
    zpd = dict(data=zp * 4 + y, expert=p)
    zmd = dict(data=zm * 4 + y, expert=p)
    qc = z * 4 + 3 - y
    home = c == s
    b_own = 4 * x + c

    def remote(src, dst, ss, rs, dev):
        return pltpu.make_async_remote_copy(src_ref=src, dst_ref=dst, send_sem=ss, recv_sem=rs,
                                            device_id=dev, device_id_type=MESH)

    def half(i):
        return pl.ds(al(i * FH), FH)

    barrier = pltpu.get_barrier_semaphore()
    for dev in (yp, zpd, zmd):
        pl.semaphore_signal(barrier, inc=1, device_id=dev, device_id_type=MESH)

    def greet(b, _):
        od = (b // 2) % 2
        yd = od * (3 - y) + (1 - od) * y

        @pl.when(b != b_own)
        def _():
            pl.semaphore_signal(barrier, inc=1, device_id=dict(data=z * 4 + yd, expert=2 * (b // 4) + b % 2), device_id_type=MESH)
        return 0

    lax.fori_loop(0, 16, greet, 0)
    pl.semaphore_wait(barrier, 18)

    hx = pl.ds(al(c * FH), FH)
    my_rows = pl.ds(al((z * 4 + yl * 2) * L), L)

    def own_copy(m):
        src = (wg_ref, wu_ref)[m]
        return remote(src.at[0, :, half(1 - c)], gu_ref.at[m, my_rows, :], ownsend_sem.at[m], own_sem.at[m], oc)

    def bounce_in(m):
        src = (wg_ref, wu_ref)[m]
        return pltpu.make_async_copy(src.at[0, :, hx], H.at[pl.ds(m * L, L), hx], loc_sem.at[m])

    def bounce_out(m):
        return pltpu.make_async_copy(H.at[pl.ds(m * L, L), hx], gu_ref.at[m, my_rows, :], own_sem.at[m])

    def nbr_copy(f, h, m):
        src = (wg_ref, wu_ref)[m]
        cols = pl.ds(al(h * FH + f * FC), FC)
        dcols = pl.ds(al(f * FC), FC)
        nyl = (3 - y) % 2
        rows = pl.ds(al((z * 4 + nyl * 2 + 1) * L), L)
        return remote(src.at[0, :, cols], gu_ref.at[m, rows, dcols], nbr_send.at[f, h, m], nbr_recv.at[f, m],
                      dict(data=qc, expert=2 * x + h))

    def nbr_start(f):
        @pl.when(jnp.logical_not(home))
        def _():
            for h in PAIR:
                for m in PAIR:
                    nbr_copy(f, h, m).start()

    PARTS = ((WA, WB), (0, WA))

    def wd0_own(i):
        o, n = PARTS[i]
        return remote(wd_ref.at[0, pl.ds(o, n), :], wdn_ref.at[z, yl, pl.ds(o, n), :],
                      wd0_send.at[i], wd0_recv.at[i], oc)

    def wd0_nbr(i):
        o, n = PARTS[i]
        return remote(wd_ref.at[0, pl.ds(o, n), :], wdn_ref.at[z, (3 - y) % 2, pl.ds(o, n), :],
                      wd0_send.at[i], wd0_recv.at[i], dict(data=qc, expert=2 * x + 1))

    def wd0_loc(i):
        o, n = PARTS[i]
        return pltpu.make_async_copy(dv.at[0, pl.ds(o, n), pl.ds(0, L)], wdn_ref.at[z, yl, pl.ds(o, n), :], wd0_recv.at[i])

    wd_in = pltpu.make_async_copy(wd_ref.at[0], dv.at[0, :, pl.ds(0, L)], loc_sem.at[2])

    @pl.when(home)
    def _():
        for m in PAIR:
            own_copy(m).start()
            bounce_in(m).start()

        @pl.when(c == 0)
        def _():
            wd_in.start()

        for m in PAIR:
            bounce_in(m).wait()
            bounce_out(m).start()

        @pl.when(c == 0)
        def _():
            wd_in.wait()
            for i in PAIR:
                wd0_loc(i).start()

        @pl.when(c == 1)
        def _():
            for i in PAIR:
                wd0_own(i).start()

    for f in range(3):
        nbr_start(f)

    def rows(zz, l, o, n):
        return pl.ds(al((zz * 4 + l * 2 + o) * L), n * L)

    def guc(f, r, i, dev):
        ref = gu_ref.at[:, r, pl.ds(al(f * FC), FC)]
        return remote(ref, ref, gu_send.at[f, i], gu_recv.at[f, i], dev)

    SENT_A = ((z, yl, 0, 2, yp), (z, 0, 0, 4, zpd), (z, 0, 0, 4, zmd), (zm, 0, 0, 2, zpd), (zp, 1, 0, 2, zmd))
    GOT_A = ((z, 1 - yl, 0, 2), (zm, 0, 0, 4), (zp, 0, 0, 4), (zo, 0, 0, 2), (zo, 1, 0, 2))
    SENT_B = ((z, yl, 0, 2, zpd), (z, yl, 0, 2, zmd), (zm, yl, 0, 1, zpd), (zp, yl, 1, 1, zmd),
              (z, yl, 0, 2, yp), (zm, yl, 0, 2, yp), (zp, yl, 0, 2, yp), (zo, yl, 0, 2, yp))
    GOT_B = ((zm, yl, 0, 2), (zp, yl, 0, 2), (zo, yl, 0, 1), (zo, yl, 1, 1),
             (z, 1 - yl, 0, 2), (zm, 1 - yl, 0, 2), (zp, 1 - yl, 0, 2), (zo, 1 - yl, 0, 2))

    def gu_put(f, sent, *ids):
        for i in ids:
            guc(f, rows(*sent[i][:4]), i, sent[i][4]).start()

    def gu_got(f, table, *ids):
        for i in ids:
            guc(f, rows(*table[i]), i, yp).wait_recv()

    def by_tree(f, do_a, do_b):
        pl.when(f % 2 == 0)(do_a)
        pl.when(f % 2 == 1)(do_b)

    def stage1(f):
        for m in PAIR:
            nbr_copy(f, 0, m).wait_recv()

        def do_a():
            gu_put(f, SENT_A, 0)

        def do_b():
            gu_put(f, SENT_B, 0, 1, 4)

        by_tree(f, do_a, do_b)

    def stage2(f):
        def do_a():
            gu_got(f, GOT_A, 0)
            gu_put(f, SENT_A, 1, 2)

        def do_b():
            gu_got(f, GOT_B, 0)
            gu_put(f, SENT_B, 2, 5)
            gu_got(f, GOT_B, 1)
            gu_put(f, SENT_B, 3, 6)

        by_tree(f, do_a, do_b)

    def stage3(f):
        def do_a():
            gu_got(f, GOT_A, 1)
            gu_put(f, SENT_A, 3)
            gu_got(f, GOT_A, 2)
            gu_put(f, SENT_A, 4)

        def do_b():
            gu_got(f, GOT_B, 2, 3)
            gu_put(f, SENT_B, 7)

        by_tree(f, do_a, do_b)

    def stage4(f):
        def do_a():
            gu_got(f, GOT_A, 3, 4)

        def do_b():
            gu_got(f, GOT_B, 4, 5, 6, 7)

        by_tree(f, do_a, do_b)

    def guc_sends(f):
        def wait(sent):
            for i, t in enumerate(sent):
                guc(f, rows(*t[:4]), i, t[4]).wait_send()

        by_tree(f, lambda: wait(SENT_A), lambda: wait(SENT_B))

    def wdc(zz, l, o, n, i, dev):
        ref = wdn_ref.at[zz, l, pl.ds(o, n), :]
        return remote(ref, ref, wd_send.at[i], wd_recv.at[i], dev)

    A = (0, WA)
    B = (WA, WB)
    B0 = (WA, WBH)
    B1 = (WA + WBH, WBH)
    SENT = ((z, yl, *B, 0, zpd), (z, yl, *B, 1, zmd), (z, yl, *B, 2, yp),
            (z, yl, *A, 3, yp), (z, yl, *A, 4, zpd), (z, yl, *A, 5, zmd),
            (z, 1 - yl, *A, 6, zpd), (z, 1 - yl, *A, 7, zmd),
            (zm, yl, *B0, 8, zpd), (zp, yl, *B1, 9, zmd),
            (zm, yl, *B, 10, yp), (zp, yl, *B, 11, yp),
            (zm, 0, *A, 12, zpd), (zp, 1, *A, 13, zmd),
            (zo, yl, *B, 14, yp))
    GOT = ((zm, yl, *B, 0, zpd), (zp, yl, *B, 1, zmd), (z, 1 - yl, *B, 2, yp),
           (z, 1 - yl, *A, 3, yp), (zm, yl, *A, 4, zpd), (zp, yl, *A, 5, zmd),
           (zm, 1 - yl, *A, 6, zpd), (zp, 1 - yl, *A, 7, zmd),
           (zo, yl, *B0, 8, zpd), (zo, yl, *B1, 9, zmd),
           (zm, 1 - yl, *B, 10, yp), (zp, 1 - yl, *B, 11, yp),
           (zo, 0, *A, 12, zpd), (zo, 1, *A, 13, zmd),
           (zo, 1 - yl, *B, 14, yp))

    def put(*ids):
        for i in ids:
            wdc(*SENT[i]).start()

    def got(*ids):
        for i in ids:
            wdc(*GOT[i]).wait_recv()

    lanes = lax.broadcasted_iota(jnp.int32, (T, L), 1)
    ids = jnp.transpose(idx_ref[...])
    gates = jnp.transpose(gate_ref[...])
    i0 = ids[:, 0:1]
    i1 = ids[:, 1:2]
    hit0 = i0 == lanes
    hit1 = i1 == lanes
    took = jnp.logical_or(hit0, hit1)
    took_f = jnp.where(took, 1.0, 0.0)
    lower = (lax.broadcasted_iota(jnp.int32, (T, T), 0) > lax.broadcasted_iota(jnp.int32, (T, T), 1))
    lower_f = jnp.where(lower, 1.0, 0.0).astype(BF16)
    count = jnp.dot(lower_f, took_f.astype(BF16), preferred_element_type=F32)
    slot_ref[...] = jnp.where(took, count, -1.0).astype(jnp.int32)
    gw_ref[...] = jnp.where(hit0, gates[:, 0:1], 0.0) + jnp.where(hit1, gates[:, 1:2], 0.0)

    def pick(e, r0, n):
        pos = lax.broadcasted_iota(jnp.int32, (n, C), 1)
        return jnp.where(slot_ref[pl.ds(r0, n), e:e + 1] == pos, 1.0, 0.0).astype(BF16)

    def tok_copy(e):
        xe, se = e // 2, e % 2
        same = jnp.where(s == se, 1, 0)
        yd = same * y + (1 - same) * (3 - y)
        o = 1 - same
        b = (x * 2 + o) * 2 + c
        return remote(S.at[e], X.at[pl.ds(pl.multiple_of(b * C, C), C), :],
                      tok_send.at[e], tok_recv.at[x * 2 + o], dict(data=z * 4 + yd, expert=2 * xe + c))

    for e in range(E):
        sel = pick(e, 0, T)
        for zz in range(4):
            r = lax.dot_general(sel, x_ref[:, zz * 512:(zz + 1) * 512], (((0,), (0,)), ((), ())),
                                preferred_element_type=F32).astype(BF16)
            for l in PAIR:
                for o in PAIR:
                    k = zz * 4 + l * 2 + o
                    n = ynat(e % 2, l, o)
                    S[e, :, k * L:(k + 1) * L] = r[:, n * L:(n + 1) * L]
        if e == 0:
            for m in PAIR:
                own_copy(m).wait_recv()
            stage1(0)
            nbr_start(3)
        if e == 3:
            stage1(1)
        if e == 6:
            stage2(0)
            nbr_start(4)

    def mine(b):
        return pl.ds(pl.multiple_of(b * C, C), C)

    X[mine(b_own), :] = S[e_own]

    def fwd(j, k):
        ref = X.at[mine(j * 2 + k), :]
        return remote(ref, ref, fwd_send.at[j], fwd_recv.at[j], oc)

    def take_tokens(o):
        for j in range(o, 8, 2):
            @pl.when(j != x * 2)
            def _():
                pltpu.make_async_copy(S.at[0], X.at[mine(j * 2 + c), :], tok_recv.at[j]).wait()
            fwd(j, c).start()

    def gu_load(f):
        return pltpu.make_async_copy(gu_ref.at[:, :, pl.ds(al(f * FC), FC)], gv.at[f % 2], gl_sem.at[f % 2])

    def gu_compute(f):
        k = f % 2
        cols = pl.ds(al(c * FH + f * FC), FC)

        def tile(r, _):
            rr = pl.ds(pl.multiple_of(r * MT, MT), MT)
            g = jnp.dot(X[rr, :], gv[k, 0], preferred_element_type=F32)
            u = jnp.dot(X[rr, :], gv[k, 1], preferred_element_type=F32)
            H[rr, cols] = (jax.nn.silu(g) * u).astype(BF16)
            return 0

        lax.fori_loop(0, NT, tile, 0)

    def h_copy(f, k):
        ref = H.at[:, pl.ds(al(k * FH + f * FC), FC)]
        return remote(ref, ref, h_send.at[f], h_recv.at[f], oc)

    def one_chunk(j):
        @pl.when(jnp.logical_or(j == 0, j >= FIRST))
        def _():
            gu_load(j).start()

        @pl.when(j + 1 < FIRST)
        def _():
            gu_load(j + 1).start()

        gu_load(j).wait()
        gu_compute(j)

        @pl.when(j > 0)
        def _():
            h_copy(j - 1, c).start()

    def done_by(i):
        return jnp.where(i < FIRST, 0, jnp.minimum(2 * (i - FIRST + 1), i - 3))

    def during(i, lo, hi, fn):
        pl.when(jnp.logical_and(i >= lo, i < hi))(fn)

    def tick(i, _):
        during(i, 2, NCH, lambda: stage1(i))
        during(i, 2, NCH - 3, lambda: nbr_start(i + 3))

        @pl.when(jnp.logical_and(i == NCH - 3, jnp.logical_not(home)))
        def _():
            for k in PAIR:
                wd0_nbr(k).start()

        during(i, 2, NCH + 1, lambda: stage2(i - 1))
        during(i, 2, E - 1, lambda: tok_copy((e_own + 1 + i) % E).start())

        @pl.when(i == NCH)
        def _():
            wd0_nbr(0).wait_recv()
            put(0, 1, 2)

        @pl.when(i == NCH + 1)
        def _():
            wd0_nbr(1).wait_recv()
            put(3, 4, 5)

        @pl.when(i == NCH + 2)
        def _():
            got(0)
            put(8, 10)
            got(1)
            put(9, 11)

        @pl.when(i == NCH + 3)
        def _():
            got(3)
            put(6, 7)

        during(i, 4, NCH + 4, lambda: stage4(i - 4))

        @pl.when(i == FIRST - 1)
        def _():
            take_tokens(0)

        @pl.when(i == FIRST)
        def _():
            take_tokens(1)
            for j in range(8):
                fwd(j, 1 - c).wait_recv()

        def chunk(j, _):
            one_chunk(j)
            return 0

        mid = jnp.minimum(done_by(i - 1) + 1, done_by(i))
        lax.fori_loop(done_by(i - 1), mid, chunk, 0)
        during(i, 2, NCH + 2, lambda: stage3(i - 2))
        lax.fori_loop(mid, done_by(i), chunk, 0)
        return 0

    tok_copy((e_own + 1) % E).start()
    tok_copy((e_own + 2) % E).start()
    lax.fori_loop(2, TICKS, tick, 0)
    h_copy(NCH - 1, c).start()

    PAIRS = (((z, 0), (z, 1)), ((zm, yl), (zp, yl)), ((zm, 1 - yl), (zp, 1 - yl)), ((zo, 0), (zo, 1)))

    def d_load(g):
        out = []
        for k, (zz, l) in enumerate(PAIRS[g]):
            if g % 3:
                lane = pl.ds(k * L, L)
            else:
                lane = pl.ds(al(((l + c) % 2) * L), L)
            out.append(pltpu.make_async_copy(wdn_ref.at[zz, l], dv.at[g % 2, :, lane], dl_sem.at[g % 2, k]))
        return out

    def places(g):
        if g % 3:
            return [(k * L, al((zz * 4 + c * (3 - 2 * s - l) + (1 - c) * (2 * s + l)) * L), L)
                    for k, (zz, l) in enumerate(PAIRS[g])]
        w = c * (1 - s) + (1 - c) * s
        return [(0, al(PAIRS[g][0][0] * 512 + w * FC), FC)]

    def out_send(g, r):
        for k in range(4):
            b = r * 4 + k
            od = k // 2
            yd = 3 - y if od else y

            @pl.when(b != b_own)
            def _():
                for lane, dst, n in places(g):
                    remote(X.at[mine(b), pl.ds(g * 256 + lane, n)], back_ref.at[e_own, :, pl.ds(dst, n)],
                           c_send.at[g], c_recv.at[g], dict(data=z * 4 + yd, expert=2 * r + k % 2)).start()

    def out_compute(g):
        for d in d_load(g):
            d.wait()

        def turn(k):
            return (x + 1 + k) % NT

        def tile(k, _):
            rr = pl.ds(pl.multiple_of(turn(k) * MT, MT), MT)
            X[rr, g * 256:(g + 1) * 256] = jnp.dot(H[rr, :], dv[g % 2], preferred_element_type=F32).astype(BF16)

            @pl.when(k > 0)
            def _():
                out_send(g, turn(k - 1))
            return 0

        lax.fori_loop(0, NT, tile, 0)
        out_send(g, turn(NT - 1))
        for lane, dst, n in places(g):
            pltpu.make_async_copy(X.at[mine(b_own), pl.ds(g * 256 + lane, n)], back_ref.at[e_own, :, pl.ds(dst, n)], c_recv.at[g]).start()

    def got_all(g):
        pltpu.make_async_copy(X.at[:, pl.ds(0, 256)], X.at[:, pl.ds(0, 256)], c_recv.at[g]).wait()

    def sent_all(g):
        pltpu.make_async_copy(X.at[pl.ds(0, 15 * C), pl.ds(0, 256)], X.at[pl.ds(0, 15 * C), pl.ds(0, 256)], c_send.at[g]).wait()

    def finish(zz):
        cols = pl.ds(al(zz * 512), 512)
        back = pltpu.make_async_copy(back_ref.at[:, :, cols], S.at[:, :, cols], bl_sem.at[0])
        back.start()
        back.wait()

        def tile(t, _):
            rr = pl.ds(pl.multiple_of(t * 256, 256), 256)
            acc = x_ref[rr, cols].astype(F32)
            for e in range(E):
                part = jnp.dot(pick(e, pl.multiple_of(t * 256, 256), 256), S[e, :, cols], preferred_element_type=F32)
                acc = acc + gw_ref[rr, e:e + 1] * part
            y_ref[rr, cols] = acc.astype(BF16)
            return 0

        lax.fori_loop(0, 2, tile, 0)

    for j in range(8):
        fwd(j, c).wait_send()
    for e in range(E):
        @pl.when(e != e_own)
        def _():
            tok_copy(e).wait_send()

    got(2)
    for d in d_load(0):
        d.start()
    for f in range(NCH):
        h_copy(f, 1 - c).wait_recv()
    out_compute(0)
    got(8, 9)
    put(14)
    got(4, 5)
    for d in d_load(1):
        d.start()
    pl.when(yl == 0)(lambda: put(12))
    pl.when(yl == 1)(lambda: put(13))
    out_compute(1)
    got(6, 7)
    pl.when(yl == 1)(lambda: put(12))
    pl.when(yl == 0)(lambda: put(13))
    got(10, 11)
    for d in d_load(2):
        d.start()
    out_compute(2)
    got_all(0)
    finish(z)
    got(12, 13, 14)
    for d in d_load(3):
        d.start()
    out_compute(3)
    got_all(1)
    got_all(2)
    finish(zm)
    finish(zp)
    got_all(3)
    finish(zo)

    def drain(f, _):
        guc_sends(f)
        h_copy(f, c).wait_send()

        @pl.when(jnp.logical_not(home))
        def _():
            for h in PAIR:
                for m in PAIR:
                    nbr_copy(f, h, m).wait_send()
        return 0

    lax.fori_loop(0, NCH, drain, 0)
    for i in range(15):
        wdc(*SENT[i]).wait_send()
    for g in range(4):
        sent_all(g)

    @pl.when(home)
    def _():
        for m in PAIR:
            own_copy(m).wait_send()

    @pl.when(jnp.logical_or(jnp.logical_not(home), c == 1))
    def _():
        for i in PAIR:
            wd0_nbr(i).wait_send()


def solution(mesh):
    tok_spec = P(("rep", "expert", "data"), None)
    wide_spec = P("expert", "data", None)
    down_spec = P("expert", None, "data")
    dma = pltpu.SemaphoreType.DMA
    two, four, eight = dma((2,)), dma((4,)), dma((E,))
    hbm = pl.BlockSpec(memory_space=pltpu.HBM)
    vmem = pl.BlockSpec(memory_space=pltpu.VMEM)

    def device_step(x_loc, idx_loc, gate_loc, wg_loc, wu_loc, wd_loc):
        out = pl.pallas_call(
            kernel,
            out_shape=(jax.ShapeDtypeStruct((T, D), BF16),
                       jax.ShapeDtypeStruct((2, D, FH), BF16),
                       jax.ShapeDtypeStruct((4, 2, FF, L), BF16),
                       jax.ShapeDtypeStruct((E, C, D), BF16)),
            in_specs=[vmem, vmem, vmem, hbm, hbm, hbm],
            out_specs=(vmem, hbm, hbm, hbm),
            scratch_shapes=[
                pltpu.VMEM((ROWS, D), BF16),
                pltpu.VMEM((ROWS, FF), BF16),
                pltpu.VMEM((2, 2, D, FC), BF16),
                pltpu.VMEM((2, FF, 256), BF16),
                pltpu.VMEM((E, C, D), BF16),
                pltpu.VMEM((T, L), jnp.int32),
                pltpu.VMEM((T, L), F32),
                two, two, dma((3,)),
                dma((NCH, 2)), dma((NCH, 2, 2)),
                dma((NCH, E)), dma((NCH, E)),
                two, two, dma((15,)), dma((15,)),
                eight, eight, eight, eight,
                dma((NCH,)), dma((NCH,)), two, dma((2, 2)),
                four, four, dma((1,)),
            ],
            compiler_params=pltpu.CompilerParams(has_side_effects=True, collective_id=0, vmem_limit_bytes=67043328),
        )(x_loc, idx_loc.T, gate_loc.T, wg_loc, wu_loc, wd_loc)
        return out[0]

    return jax.shard_map(device_step, mesh=mesh, in_specs=(tok_spec, tok_spec, tok_spec, wide_spec, wide_spec, down_spec), out_specs=tok_spec, check_vma=False)
```
